256 devices in a mesh: group: 2 (over core), dp: 8 (over z_lo, x), mp: 16 (over y, z_hi).
Axes of the slice: x: 4, y: 4, z: 8 (z_hi: 4, z_lo: 2; z = z_hi * 2 + z_lo), core: 2. Of those that a mesh axis runs over, the one named last changes fastest.
Arguments:
- latents: float32 [16, 320, 2432], P(('group', 'dp')), may hold values from -6 to 6
- noise: bfloat16 [16, 2, 320, 2432], P(('group', 'dp')), may hold values from -6 to 6
- ref_velocity: bfloat16 [16, 2, 320, 2432], P(('group', 'dp')), may hold values from -6 to 6
- start_step: int32 [16], P(('group', 'dp')), may hold values from 1 to 6
- advantages: float32 [16], P(('group', 'dp')), may hold values from -4 to 4
- behaviour_gap: float32 [16, 2], P(('group', 'dp')), may hold values from -0.4 to 0.4
- modulation: float32 [10, 2, 2432], replicated, may hold values from -3 to 3
- w_in: bfloat16 [2432, 9728], P(('group', 'dp'), 'mp'), may hold values from -6 to 6
- w_down: bfloat16 [2432, 9728], P(('group', 'dp'), 'mp'), may hold values from -6 to 6
Outputs:
- final_latents: float32 [16, 320, 2432], P(('group', 'dp'))
- new_w_in: bfloat16 [2432, 9728], P(('group', 'dp'), 'mp')
- new_w_down: bfloat16 [2432, 9728], P(('group', 'dp'), 'mp')
The draws below stay inside these ranges and needn't reach their ends.
Inputs may be any that keep to these rules, and one draw needn't show every extreme that they name: `start_step`: the second step of an image is at the next plan position.
All inputs are finite; a program needn't handle non-finite values.
Results may differ from the reference program's by a relative error of at most 0.014.
Values may be sent and summed in bfloat16 or wider, within the bound.
No kernel may reach another device: no remote copies, remote signals or barrier semaphores. Data moves between devices by JAX's collectives and lax.ppermute only.
A program may use at most 128 MiB of HBM per device.

```python
import math
import jax
import jax.numpy as jnp
from jax import lax

D = 2432
FF = 9728
LEN = 320
SCHED = 10
IMAGES = 16


def set_ends(array, rng, least, largest):
    index_at = [jax.random.randint(jax.random.fold_in(rng, axis), (), 0, length) for axis, length in enumerate(array.shape)]
    main_axis = array.shape.index(max(array.shape))
    neighbour = index_at[:main_axis] + [(index_at[main_axis] + 1) % array.shape[main_axis]] + index_at[main_axis + 1:]
    return array.at[tuple(index_at)].set(least).at[tuple(neighbour)].set(largest)


def block_levels(key, shape, cuts, low, largest):
    factor_of, own = 1.0, jax.random.fold_in(key, 6)
    for axis_at, parts in cuts:
        heights = jnp.exp(jax.random.uniform(jax.random.fold_in(own, axis_at), (parts,), jnp.float32, low / len(cuts), largest / len(cuts)))
        factor_of = factor_of * jnp.repeat(heights, shape[axis_at] // parts).reshape([-1 if axis == axis_at else 1 for axis in range(len(shape))])
    return factor_of


def centred(key, extent, spread, reach, split=(), held_as=jnp.bfloat16):
    factor_of = block_levels(key, extent, split, -0.22, 0.18) if split else 1.0
    result = jax.random.normal(key, extent, jnp.float32) * spread * factor_of
    return jnp.minimum(jnp.maximum(result, -reach), reach).astype(held_as)


def setup_inputs(seed: int = 0) -> dict:
    seeds = jax.random.split(jax.random.key(seed), 10)
    latents = centred(seeds[0], (IMAGES, LEN, D), 1.0, 6.0, ((0, 16),), jnp.float32)
    noise = centred(seeds[1], (IMAGES, 2, LEN, D), 1.0, 6.0, ((0, 16),))
    ref_velocity = centred(seeds[2], (IMAGES, 2, LEN, D), 1.0, 6.0, ((0, 16),))
    start_step = set_ends(jax.random.randint(seeds[3], (IMAGES,), 1, 7), jax.random.fold_in(seeds[3], 1), 1, 6).astype(jnp.int32)
    advantages = centred(seeds[4], (IMAGES,), 1.0, 4.0, ((0, 16),), jnp.float32)
    behaviour_gap = jnp.clip(jax.random.uniform(seeds[5], (IMAGES, 2), jnp.float32, -0.4, 0.4) * block_levels(seeds[5], (IMAGES, 2), ((0, 16),), -0.4, 0.0), -0.4, 0.4)
    modulation = centred(seeds[6], (SCHED, 2, D), 0.5, 3.0, (), jnp.float32)
    w_in = centred(seeds[7], (D, FF), 1.0, 6.0, ((0, 16), (1, 16)))
    w_down = centred(seeds[8], (D, FF), 1.0, 6.0, ((0, 16), (1, 16)))
    return {"latents": latents, "noise": noise, "ref_velocity": ref_velocity, "start_step": start_step, "advantages": advantages, "behaviour_gap": behaviour_gap, "modulation": modulation, "w_in": w_in, "w_down": w_down}


NOISE_SLOPE = 0.7
CLIP_RANGE = 0.2
GELU_COEF = 0.7978845608028654
GELU_CUBE = 0.044715
HIGH_PREC = lax.Precision.HIGHEST

def gelu_parts(pre_act):
    tangent = jnp.tanh(GELU_COEF * (pre_act + GELU_CUBE * pre_act * pre_act * pre_act))
    activation = 0.5 * pre_act * (1.0 + tangent)
    gelu_slope = 0.5 * (1.0 + tangent) + 0.5 * pre_act * (1.0 - tangent * tangent) * GELU_COEF * (1.0 + 3.0 * GELU_CUBE * pre_act * pre_act)
    return (activation, gelu_slope)

def reference(latents, noise, ref_velocity, start_step, advantages, behaviour_gap, modulation, w_in, w_down):
    model_width = latents.shape[2]
    hidden_width = w_in.shape[1]
    step_len = 1.0 / SCHED
    vel_coef = 1.0 + 0.5 * NOISE_SLOPE * NOISE_SLOPE
    latent_now = jnp.transpose(latents, (1, 0, 2))
    w_in_wide = w_in.astype(jnp.float32)
    w_down_wide = w_down.astype(jnp.float32)
    grad_in = jnp.zeros((model_width, hidden_width), jnp.float32)
    grad_down = jnp.zeros((model_width, hidden_width), jnp.float32)
    for step_num in range(2):
        sched_index = start_step + step_num
        time_now = 1.0 - sched_index.astype(jnp.float32) / SCHED
        onehot = (sched_index[:, None] == jnp.arange(SCHED, dtype=jnp.int32)[None, :]).astype(jnp.float32)
        mod_rows = jnp.einsum('is,scd->icd', onehot, modulation, precision=HIGH_PREC)
        normed = latent_now * lax.rsqrt(lax.optimization_barrier(jnp.mean(latent_now * latent_now, axis=2, keepdims=True)) + 1e-06)
        inputs = (normed * (1.0 + mod_rows[None, :, 1, :]) + mod_rows[None, :, 0, :]).astype(jnp.bfloat16)
        pre_act = jnp.einsum('lid,df->lif', inputs.astype(jnp.float32), w_in_wide, precision=HIGH_PREC) / math.sqrt(model_width)
        activation, gelu_slope = gelu_parts(pre_act)
        hidden = activation.astype(jnp.bfloat16)
        velocity = jnp.einsum('lif,df->lid', hidden.astype(jnp.float32), w_down_wide, precision=HIGH_PREC) / math.sqrt(hidden_width)
        noise_level = (NOISE_SLOPE * jnp.sqrt(time_now / (1.0 - time_now)))[None, :, None]
        drift_x = (0.5 * NOISE_SLOPE * NOISE_SLOPE / (1.0 - time_now))[None, :, None]
        eps_draw = jnp.transpose(noise[:, step_num], (1, 0, 2)).astype(jnp.float32)
        ref_vel = jnp.transpose(ref_velocity[:, step_num], (1, 0, 2)).astype(jnp.float32)
        step_mean = latent_now * (1.0 - step_len * drift_x) - step_len * vel_coef * velocity
        latent_next = step_mean + noise_level * math.sqrt(step_len) * eps_draw
        policy_ratio = jnp.exp(behaviour_gap[:, step_num])
        active = (advantages >= 0.0) & (policy_ratio <= 1.0 + CLIP_RANGE) | (advantages < 0.0) & (policy_ratio >= 1.0 - CLIP_RANGE)
        pg_coef = jnp.where(active, policy_ratio * advantages, jnp.zeros_like(advantages))[None, :, None]
        vel_grad = (pg_coef * vel_coef * math.sqrt(step_len) * eps_draw / noise_level + vel_coef * vel_coef * step_len * (velocity - ref_vel) / (noise_level * noise_level)).astype(jnp.bfloat16)
        hid_grad = jnp.einsum('lid,df->lif', vel_grad.astype(jnp.float32), w_down_wide, precision=HIGH_PREC) / math.sqrt(hidden_width)
        pre_grad = (hid_grad * gelu_slope).astype(jnp.bfloat16)
        grad_in = grad_in + jnp.einsum('lid,lif->df', inputs.astype(jnp.float32), pre_grad.astype(jnp.float32), precision=HIGH_PREC) / math.sqrt(model_width)
        grad_down = grad_down + jnp.einsum('lid,lif->df', vel_grad.astype(jnp.float32), hidden.astype(jnp.float32), precision=HIGH_PREC) / math.sqrt(hidden_width)
        latent_now = latent_next
    total = jnp.sum(grad_in * grad_in) + jnp.sum(grad_down * grad_down)
    grad_rms = jnp.sqrt(total / (2.0 * model_width * hidden_width) + 1e-06)
    new_w_in = (w_in_wide - grad_in / grad_rms).astype(jnp.bfloat16)
    new_w_down = (w_down_wide - grad_down / grad_rms).astype(jnp.bfloat16)
    return (jnp.transpose(latent_now, (1, 0, 2)), new_w_in, new_w_down)
```

```python
import math

import jax
import jax.numpy as jnp
from jax import lax
from jax.sharding import Mesh
from jax.sharding import PartitionSpec as P

SCHED = 10
MP = ("mp_0", "mp_1")
GROUP_DP = ("group", "dp_0", "dp_1")
GROUP_DP_MP = ("group", "dp_0", "dp_1", "mp_0", "mp_1")


NOISE_SLOPE = 0.7
CLIP_RANGE = 0.2
GELU_COEF = 0.7978845608028654
GELU_CUBE = 0.044715
HIGH_PREC = lax.Precision.HIGHEST


def to_shifted(array, axis, shift):
    peers = lax.axis_size(axis)
    return lax.ppermute(array, axis, [(i, (i + shift) % peers) for i in range(peers)])


def share_for(array, axis, shift, dim):
    peers = lax.axis_size(axis)
    length = array.shape[dim] // peers
    at = (lax.axis_index(axis) + shift) % peers
    return lax.dynamic_slice_in_dim(array, at * length, length, axis=dim)


def sum_shares(array, axis, dim):
    peers = lax.axis_size(axis)
    got = [
        to_shifted(share_for(array, axis, s, dim), axis, s)
        for s in sorted(range(1, peers), key=lambda s: -min(s, peers - s))
    ]
    total = share_for(array, axis, 0, dim).astype(jnp.float32)
    for piece in got:
        total = total + piece.astype(jnp.float32)
    return total


def join_shares(share, axis, dim):
    peers = lax.axis_size(axis)
    me = lax.axis_index(axis)
    if peers == 2:
        other = to_shifted(share, axis, 1)
        first = me == 0
        return jnp.concatenate(
            [jnp.where(first, share, other), jnp.where(first, other, share)], axis=dim
        )
    length = share.shape[dim]
    shifts = sorted(range(1, peers), key=lambda s: -min(s, peers - s))
    got = [to_shifted(share, axis, s) for s in shifts]
    shape = list(share.shape)
    shape[dim] = length * peers
    whole = jnp.zeros(shape, share.dtype)
    for s, piece in zip([0] + shifts, [share] + got):
        at = (me - s) % peers
        whole = lax.dynamic_update_slice_in_dim(whole, piece, at * length, axis=dim)
    return whole


def gathered_weights(w_in, w_down):
    rows, units = w_in.shape
    in_x = join_shares(w_in, "dp_1", 0)
    down_z = join_shares(w_down[None], "dp_0", 0)
    in_xz = join_shares(in_x, "dp_0", 0)
    down_zx = join_shares(down_z[:, None], "dp_1", 1)
    w_in_full = join_shares(in_xz, "group", 0)
    w_down_full = join_shares(down_zx.reshape(-1, units), "group", 0)
    return (w_in_full, w_down_full)


def total_over_hidden(partial):
    mine = sum_shares(partial, "mp_0", 0).astype(jnp.bfloat16)
    mine = sum_shares(mine, "mp_1", 0).astype(jnp.bfloat16)
    return join_shares(join_shares(mine, "mp_1", 0), "mp_0", 0)


def down_to_owner(grad):
    half = sum_shares(grad, "group", 0).astype(jnp.bfloat16)
    half = sum_shares(half, "dp_0", 0).astype(jnp.bfloat16)
    return sum_shares(half, "dp_1", 0)


def in_to_owner(grad):
    half = sum_shares(grad, "group", 0).astype(jnp.bfloat16)
    half = half.reshape(2, 4, -1, grad.shape[1])
    half = sum_shares(half, "dp_1", 1).astype(jnp.bfloat16)
    return sum_shares(half, "dp_0", 0)[0, 0]


def sum_over_all(value):
    devices = lax.axis_size(GROUP_DP_MP)
    parts = lax.all_to_all(
        jnp.full((devices, 128), value, jnp.float32), GROUP_DP_MP, 0, 0, tiled=True
    )
    return jnp.sum(parts[:, 0])


def gelu_parts(pre_act):
    tangent = jnp.tanh(GELU_COEF * (pre_act + GELU_CUBE * pre_act * pre_act * pre_act))
    activation = 0.5 * pre_act * (1.0 + tangent)
    gelu_slope = 0.5 * (1.0 + tangent) + 0.5 * pre_act * (1.0 - tangent * tangent) * GELU_COEF * (
        1.0 + 3.0 * GELU_CUBE * pre_act * pre_act
    )
    return (activation, gelu_slope)


def on_device(
    latents, noise, ref_velocity, start_step, advantages, behaviour_gap, modulation, w_in, w_down
):
    model_width = latents.shape[2]
    shard_units = w_in.shape[1]
    hidden_width = shard_units * lax.axis_size(MP)
    step_len = 1.0 / SCHED
    vel_coef = 1.0 + 0.5 * NOISE_SLOPE * NOISE_SLOPE
    w_in_full, w_down_full = gathered_weights(w_in, w_down)
    latent_now = latents
    grad_in = grad_down = 0.0
    for step_num in range(2):
        sched_index = start_step + step_num
        time_now = 1.0 - sched_index.astype(jnp.float32) / SCHED
        onehot = (sched_index[:, None] == jnp.arange(SCHED, dtype=jnp.int32)[None, :]).astype(
            jnp.float32
        )
        mod_rows = jnp.einsum("is,scd->icd", onehot, modulation, precision=HIGH_PREC)
        normed = latent_now * lax.rsqrt(
            jnp.mean(latent_now * latent_now, axis=2, keepdims=True) + 1e-06
        )
        inputs = (normed * (1.0 + mod_rows[:, None, 1, :]) + mod_rows[:, None, 0, :]).astype(
            jnp.bfloat16
        )
        pre_act = jnp.einsum(
            "ild,df->ilf", inputs, w_in_full, preferred_element_type=jnp.float32
        ) / math.sqrt(model_width)
        activation, gelu_slope = gelu_parts(pre_act)
        hidden = activation.astype(jnp.bfloat16)
        partial_vel = jnp.einsum(
            "ilf,df->ild", hidden, w_down_full, preferred_element_type=jnp.float32
        ) / math.sqrt(hidden_width)
        velocity = total_over_hidden(partial_vel.astype(jnp.bfloat16)[0])[None].astype(jnp.float32)
        noise_level = (NOISE_SLOPE * jnp.sqrt(time_now / (1.0 - time_now)))[:, None, None]
        drift_x = (0.5 * NOISE_SLOPE * NOISE_SLOPE / (1.0 - time_now))[:, None, None]
        eps_draw = noise[:, step_num].astype(jnp.float32)
        ref_vel = ref_velocity[:, step_num].astype(jnp.float32)
        step_mean = latent_now * (1.0 - step_len * drift_x) - step_len * vel_coef * velocity
        latent_now = step_mean + noise_level * math.sqrt(step_len) * eps_draw
        policy_ratio = jnp.exp(behaviour_gap[:, step_num])
        active = (advantages >= 0.0) & (policy_ratio <= 1.0 + CLIP_RANGE) | (advantages < 0.0) & (
            policy_ratio >= 1.0 - CLIP_RANGE
        )
        pg_coef = jnp.where(active, policy_ratio * advantages, jnp.zeros_like(advantages))[
            :, None, None
        ]
        vel_grad = (
            pg_coef * vel_coef * math.sqrt(step_len) * eps_draw / noise_level
            + vel_coef * vel_coef * step_len * (velocity - ref_vel) / (noise_level * noise_level)
        ).astype(jnp.bfloat16)
        grad_down = grad_down + jnp.einsum(
            "ild,ilf->df", vel_grad, hidden, preferred_element_type=jnp.float32
        )
        hid_grad = jnp.einsum(
            "ild,df->ilf", vel_grad, w_down_full, preferred_element_type=jnp.float32
        ) / math.sqrt(hidden_width)
        pre_grad = (hid_grad * gelu_slope).astype(jnp.bfloat16)
        grad_in = grad_in + jnp.einsum(
            "ild,ilf->df", inputs, pre_grad, preferred_element_type=jnp.float32
        )
    down_mine = down_to_owner((grad_down / math.sqrt(hidden_width)).astype(jnp.bfloat16))
    in_mine = in_to_owner((grad_in / math.sqrt(model_width)).astype(jnp.bfloat16))
    total = sum_over_all(jnp.sum(in_mine * in_mine) + jnp.sum(down_mine * down_mine))
    grad_rms = jnp.sqrt(total / (2.0 * model_width * hidden_width) + 1e-06)
    new_in = (w_in.astype(jnp.float32) - in_mine / grad_rms).astype(jnp.bfloat16)
    new_down = (w_down.astype(jnp.float32) - down_mine / grad_rms).astype(jnp.bfloat16)
    return (latent_now, new_in, new_down)


def solution(mesh):
    finer = Mesh(
        mesh.devices.reshape(mesh.shape["group"], 2, 4, 4, 4),
        ("group", "dp_0", "dp_1", "mp_0", "mp_1"),
    )
    placed = (
        P(GROUP_DP, None, None),
        P(GROUP_DP, None, None, None),
        P(GROUP_DP, None, None, None),
        P(GROUP_DP),
        P(GROUP_DP),
        P(GROUP_DP, None),
        P(),
        P(GROUP_DP, MP),
        P(GROUP_DP, MP),
    )
    return jax.shard_map(
        on_device,
        mesh=finer,
        in_specs=placed,
        out_specs=(P(GROUP_DP, None, None), P(GROUP_DP, MP), P(GROUP_DP, MP)),
        check_vma=False,
    )
```

```python
import functools
import math

import jax
import jax.numpy as jnp
from jax import lax
from jax.experimental import pallas as pl
from jax.experimental.pallas import tpu as pltpu
from jax.sharding import Mesh
from jax.sharding import PartitionSpec as P

SCHED = 10
MP = ("mp_0", "mp_1")
GROUP_DP = ("group", "dp_0", "dp_1")
GROUP_DP_MP = ("group", "dp_0", "dp_1", "mp_0", "mp_1")


NOISE_SLOPE = 0.7
CLIP_RANGE = 0.2
GELU_COEF = 0.7978845608028654
GELU_CUBE = 0.044715
HIGH_PREC = lax.Precision.HIGHEST


def to_shifted(array, axis, shift):
    peers = lax.axis_size(axis)
    return lax.ppermute(array, axis, [(i, (i + shift) % peers) for i in range(peers)])


def share_for(array, axis, shift, dim):
    peers = lax.axis_size(axis)
    length = array.shape[dim] // peers
    at = (lax.axis_index(axis) + shift) % peers
    return lax.dynamic_slice_in_dim(array, at * length, length, axis=dim)


def sum_shares(array, axis, dim):
    peers = lax.axis_size(axis)
    got = [
        to_shifted(share_for(array, axis, s, dim), axis, s)
        for s in sorted(range(1, peers), key=lambda s: -min(s, peers - s))
    ]
    total = share_for(array, axis, 0, dim).astype(jnp.float32)
    for piece in got:
        total = total + piece.astype(jnp.float32)
    return total


def join_shares(share, axis, dim):
    peers = lax.axis_size(axis)
    me = lax.axis_index(axis)
    if peers == 2:
        other = to_shifted(share, axis, 1)
        first = me == 0
        return jnp.concatenate(
            [jnp.where(first, share, other), jnp.where(first, other, share)], axis=dim
        )
    length = share.shape[dim]
    shifts = sorted(range(1, peers), key=lambda s: -min(s, peers - s))
    got = [to_shifted(share, axis, s) for s in shifts]
    shape = list(share.shape)
    shape[dim] = length * peers
    whole = jnp.zeros(shape, share.dtype)
    for s, piece in zip([0] + shifts, [share] + got):
        at = (me - s) % peers
        whole = lax.dynamic_update_slice_in_dim(whole, piece, at * length, axis=dim)
    return whole


def gathered_weights(w_in, w_down):
    rows, units = w_in.shape
    in_x = join_shares(w_in, "dp_1", 0)
    down_z = join_shares(w_down[None], "dp_0", 0)
    in_xz = join_shares(in_x, "dp_0", 0)
    down_zx = join_shares(down_z[:, None], "dp_1", 1)
    w_in_full = join_shares(in_xz, "group", 0)
    w_down_full = join_shares(down_zx.reshape(-1, units), "group", 0)
    return (w_in_full, w_down_full)


LANES = 128


def picked(pieces, me, c):
    r = (me - c) % len(pieces)
    out = pieces[-1]
    for k in range(len(pieces) - 2, -1, -1):
        out = jnp.where(r == k, pieces[k], out)
    return out


def total_over_hidden(partial):
    mine = sum_shares(partial, "mp_0", 0)
    width = mine.shape[1]
    peers = lax.axis_size("mp_1")
    spare = -width % (peers * LANES)
    mine = jnp.pad(mine, ((0, 0), (0, spare))).astype(jnp.bfloat16)
    piece = sum_shares(mine, "mp_1", 1).astype(jnp.bfloat16)
    pieces = [piece] + [to_shifted(piece, "mp_1", s) for s in (1, 2, 3)]
    me = lax.axis_index("mp_1")
    rows = jnp.concatenate([picked(pieces, me, c) for c in range(peers)], axis=1)
    return join_shares(rows[:, :width], "mp_0", 0)


def grad_kernel(scale, side_ref, l0, l1, r0, r1, mine, other, whole, sems):
    right = jnp.concatenate([r0[...], r1[...]], axis=0)
    depth = l0.shape[1]
    step = 5 * LANES
    for at in range(0, depth, step):
        end = min(at + step, depth)
        left = jnp.concatenate([l0[:, at:end], l1[:, at:end]], axis=0)
        block = lax.dot_general(
            left, right, (((0,), (0,)), ((), ())), preferred_element_type=jnp.float32
        )
        whole[at:end, :] = (block * scale).astype(jnp.bfloat16)
    half = depth // 2
    side = side_ref[0]
    copies = (
        pltpu.make_async_copy(
            whole.at[pl.ds(pl.multiple_of((1 - side) * half, 16), half)], other, sems.at[0]
        ),
        pltpu.make_async_copy(
            whole.at[pl.ds(pl.multiple_of(side * half, 16), half)], mine, sems.at[1]
        ),
    )
    for copy in copies:
        copy.start()
    for copy in copies:
        copy.wait()


def grad_halves(l0, l1, r0, r1, scale):
    depth, units = l0.shape[1], r0.shape[1]
    half = jax.ShapeDtypeStruct((depth // 2, units), jnp.bfloat16)
    vmem = pl.BlockSpec(memory_space=pltpu.VMEM)
    return pl.pallas_call(
        functools.partial(grad_kernel, scale),
        out_shape=(half, half),
        in_specs=[pl.BlockSpec(memory_space=pltpu.SMEM)] + [vmem] * 4,
        out_specs=(pl.BlockSpec(memory_space=pl.ANY),) * 2,
        scratch_shapes=[
            pltpu.VMEM((depth, units), jnp.bfloat16),
            pltpu.SemaphoreType.DMA((2,)),
        ],
        compiler_params=pltpu.CompilerParams(vmem_limit_bytes=24 << 20),
        cost_estimate=pl.CostEstimate(
            flops=4 * depth * units * l0.shape[0], bytes_accessed=8 << 20, transcendentals=0
        ),
    )(lax.axis_index("group")[None], l0, l1, r0, r1)


def over_cores(mine, other):
    got = to_shifted(other, "group", 1)
    return (mine.astype(jnp.float32) + got.astype(jnp.float32)).astype(jnp.bfloat16)


def down_to_owner(mine, other):
    half = over_cores(mine, other)
    half = sum_shares(half, "dp_0", 0).astype(jnp.bfloat16)
    return sum_shares(half, "dp_1", 0)


def in_to_owner(mine, other):
    half = over_cores(mine, other)
    rows = half.shape[0] // 8
    me = lax.axis_index("dp_1")

    def share(s):
        at = (me + s) % 4
        return jnp.concatenate(
            [
                lax.dynamic_slice_in_dim(half, (z * 4 + at) * rows, rows, axis=0)
                for z in range(2)
            ],
            axis=0,
        )

    got = [to_shifted(share(s), "dp_1", s) for s in (2, 1, 3)]
    total = share(0).astype(jnp.float32)
    for piece in got:
        total = total + piece.astype(jnp.float32)
    return sum_shares(total.astype(jnp.bfloat16), "dp_0", 0)


def sum_over_all(value):
    near = ("group", "dp_0")
    line = jnp.full((8, LANES), value, jnp.float32)
    parts = [lax.ppermute(line, near, [(i, i ^ s) for i in range(4)]) for s in (3, 2, 1)]
    line = line + parts[0] + parts[1] + parts[2]
    far = ("dp_1", "mp_0", "mp_1")
    devices = lax.axis_size(far)
    got = lax.all_to_all(
        jnp.broadcast_to(line[:1], (devices, LANES)), far, 0, 0, tiled=True
    )
    return jnp.sum(got[:, 0])


def gelu_parts(pre_act):
    tangent = jnp.tanh(GELU_COEF * (pre_act + GELU_CUBE * pre_act * pre_act * pre_act))
    activation = 0.5 * pre_act * (1.0 + tangent)
    gelu_slope = 0.5 * (1.0 + tangent) + 0.5 * pre_act * (1.0 - tangent * tangent) * GELU_COEF * (
        1.0 + 3.0 * GELU_CUBE * pre_act * pre_act
    )
    return (activation, gelu_slope)


def on_device(
    latents, noise, ref_velocity, start_step, advantages, behaviour_gap, modulation, w_in, w_down
):
    model_width = latents.shape[2]
    shard_units = w_in.shape[1]
    hidden_width = shard_units * lax.axis_size(MP)
    step_len = 1.0 / SCHED
    vel_coef = 1.0 + 0.5 * NOISE_SLOPE * NOISE_SLOPE
    w_in_full, w_down_full = gathered_weights(w_in, w_down)
    latent_now = latents
    lefts = []
    downs = []
    for step_num in range(2):
        sched_index = start_step + step_num
        time_now = 1.0 - sched_index.astype(jnp.float32) / SCHED
        onehot = (sched_index[:, None] == jnp.arange(SCHED, dtype=jnp.int32)[None, :]).astype(
            jnp.float32
        )
        mod_rows = jnp.einsum("is,scd->icd", onehot, modulation, precision=HIGH_PREC)
        normed = latent_now * lax.rsqrt(
            jnp.mean(latent_now * latent_now, axis=2, keepdims=True) + 1e-06
        )
        inputs = (normed * (1.0 + mod_rows[:, None, 1, :]) + mod_rows[:, None, 0, :]).astype(
            jnp.bfloat16
        )
        pre_act = jnp.einsum(
            "ild,df->ilf", inputs, w_in_full, preferred_element_type=jnp.float32
        ) / math.sqrt(model_width)
        activation, gelu_slope = gelu_parts(pre_act)
        hidden = activation.astype(jnp.bfloat16)
        partial_vel = jnp.einsum(
            "ilf,df->ild", hidden, w_down_full, preferred_element_type=jnp.float32
        ) / math.sqrt(hidden_width)
        velocity = total_over_hidden(partial_vel.astype(jnp.bfloat16)[0])[None].astype(jnp.float32)
        noise_level = (NOISE_SLOPE * jnp.sqrt(time_now / (1.0 - time_now)))[:, None, None]
        drift_x = (0.5 * NOISE_SLOPE * NOISE_SLOPE / (1.0 - time_now))[:, None, None]
        eps_draw = noise[:, step_num].astype(jnp.float32)
        ref_vel = ref_velocity[:, step_num].astype(jnp.float32)
        step_mean = latent_now * (1.0 - step_len * drift_x) - step_len * vel_coef * velocity
        latent_now = step_mean + noise_level * math.sqrt(step_len) * eps_draw
        policy_ratio = jnp.exp(behaviour_gap[:, step_num])
        active = (advantages >= 0.0) & (policy_ratio <= 1.0 + CLIP_RANGE) | (advantages < 0.0) & (
            policy_ratio >= 1.0 - CLIP_RANGE
        )
        pg_coef = jnp.where(active, policy_ratio * advantages, jnp.zeros_like(advantages))[
            :, None, None
        ]
        vel_grad = (
            pg_coef * vel_coef * math.sqrt(step_len) * eps_draw / noise_level
            + vel_coef * vel_coef * step_len * (velocity - ref_vel) / (noise_level * noise_level)
        ).astype(jnp.bfloat16)
        vel_grad = lax.optimization_barrier(vel_grad)
        hid_grad = jnp.einsum(
            "ild,df->ilf", vel_grad, w_down_full, preferred_element_type=jnp.float32
        ) / math.sqrt(hidden_width)
        pre_grad = (hid_grad * gelu_slope).astype(jnp.bfloat16)
        downs += [vel_grad[0], lax.optimization_barrier(hidden)[0]]
        lefts += [inputs[0], lax.optimization_barrier(pre_grad)[0]]
    down_mine = down_to_owner(
        *grad_halves(downs[0], downs[2], downs[1], downs[3], 1.0 / math.sqrt(hidden_width))
    )
    in_mine = in_to_owner(
        *grad_halves(lefts[0], lefts[2], lefts[1], lefts[3], 1.0 / math.sqrt(model_width))
    )
    total = sum_over_all(jnp.sum(in_mine * in_mine) + jnp.sum(down_mine * down_mine))
    grad_rms = jnp.sqrt(total / (2.0 * model_width * hidden_width) + 1e-06)
    new_in = (w_in.astype(jnp.float32) - in_mine / grad_rms).astype(jnp.bfloat16)
    new_down = (w_down.astype(jnp.float32) - down_mine / grad_rms).astype(jnp.bfloat16)
    return (latent_now, new_in, new_down)


def solution(mesh):
    finer = Mesh(
        mesh.devices.reshape(mesh.shape["group"], 2, 4, 4, 4),
        ("group", "dp_0", "dp_1", "mp_0", "mp_1"),
    )
    placed = (
        P(GROUP_DP, None, None),
        P(GROUP_DP, None, None, None),
        P(GROUP_DP, None, None, None),
        P(GROUP_DP),
        P(GROUP_DP),
        P(GROUP_DP, None),
        P(),
        P(GROUP_DP, MP),
        P(GROUP_DP, MP),
    )
    return jax.shard_map(
        on_device,
        mesh=finer,
        in_specs=placed,
        out_specs=(P(GROUP_DP, None, None), P(GROUP_DP, MP), P(GROUP_DP, MP)),
        check_vma=False,
    )
```

```python
import functools
import math

import jax
import jax.numpy as jnp
from jax import lax
from jax.experimental import pallas as pl
from jax.experimental.pallas import tpu as pltpu
from jax.sharding import Mesh
from jax.sharding import PartitionSpec as P

SCHED = 10
MP = ("mp_0", "mp_1")
GROUP_DP = ("group", "dp_0", "dp_1")
GROUP_DP_MP = ("group", "dp_0", "dp_1", "mp_0", "mp_1")


NOISE_SLOPE = 0.7
CLIP_RANGE = 0.2
GELU_COEF = 0.7978845608028654
GELU_CUBE = 0.044715
HIGH_PREC = lax.Precision.HIGHEST


def to_shifted(array, axis, shift):
    peers = lax.axis_size(axis)
    return lax.ppermute(array, axis, [(i, (i + shift) % peers) for i in range(peers)])


def share_for(array, axis, shift, dim):
    peers = lax.axis_size(axis)
    length = array.shape[dim] // peers
    at = (lax.axis_index(axis) + shift) % peers
    return lax.dynamic_slice_in_dim(array, at * length, length, axis=dim)


def sum_shares(array, axis, dim):
    peers = lax.axis_size(axis)
    got = [
        to_shifted(share_for(array, axis, s, dim), axis, s)
        for s in sorted(range(1, peers), key=lambda s: -min(s, peers - s))
    ]
    total = share_for(array, axis, 0, dim).astype(jnp.float32)
    for piece in got:
        total = total + piece.astype(jnp.float32)
    return total


def join_shares(share, axis, dim):
    peers = lax.axis_size(axis)
    me = lax.axis_index(axis)
    if peers == 2:
        other = to_shifted(share, axis, 1)
        first = me == 0
        return jnp.concatenate(
            [jnp.where(first, share, other), jnp.where(first, other, share)], axis=dim
        )
    length = share.shape[dim]
    shifts = sorted(range(1, peers), key=lambda s: -min(s, peers - s))
    got = [to_shifted(share, axis, s) for s in shifts]
    shape = list(share.shape)
    shape[dim] = length * peers
    whole = jnp.zeros(shape, share.dtype)
    for s, piece in zip([0] + shifts, [share] + got):
        at = (me - s) % peers
        whole = lax.dynamic_update_slice_in_dim(whole, piece, at * length, axis=dim)
    return whole


def gathered_weights(w_in, w_down):
    rows, units = w_in.shape
    in_x = join_shares(w_in, "dp_1", 0)
    down_z = join_shares(w_down[None], "dp_0", 0)
    in_xz = join_shares(in_x, "dp_0", 0)
    down_zx = join_shares(down_z[:, None], "dp_1", 1)
    w_in_full = join_shares(in_xz, "group", 0)
    w_down_full = join_shares(down_zx.reshape(-1, units), "group", 0)
    return (w_in_full, w_down_full)


LANES = 128


def picked(pieces, me, c):
    r = (me - c) % len(pieces)
    out = pieces[-1]
    for k in range(len(pieces) - 2, -1, -1):
        out = jnp.where(r == k, pieces[k], out)
    return out


ORDER = (0, 1, 3, 2)


def to_relative(array, axis, dim):
    length = array.shape[dim] // len(ORDER)
    me = lax.axis_index(axis)
    return jnp.concatenate(
        [
            lax.dynamic_slice_in_dim(array, (me - s) % len(ORDER) * length, length, axis=dim)
            for s in ORDER
        ],
        axis=dim,
    )


def to_absolute(array, axis, dim):
    length = array.shape[dim] // len(ORDER)
    me = lax.axis_index(axis)
    parts = []
    for c in range(len(ORDER)):
        s = (me - c) % len(ORDER)
        at = s ^ (s >> 1)
        parts.append(lax.dynamic_slice_in_dim(array, at * length, length, axis=dim))
    return jnp.concatenate(parts, axis=dim)


def over_z(mine):
    width = mine.shape[1]
    peers = lax.axis_size("mp_1")
    spare = -width % (peers * LANES)
    mine = jnp.pad(mine, ((0, 0), (0, spare))).astype(jnp.bfloat16)
    piece = sum_shares(mine, "mp_1", 1).astype(jnp.bfloat16)
    pieces = [piece] + [to_shifted(piece, "mp_1", s) for s in (1, 2, 3)]
    me = lax.axis_index("mp_1")
    rows = jnp.concatenate([picked(pieces, me, c) for c in range(peers)], axis=1)
    return rows[:, :width]


def added(own, pieces):
    total = own.astype(jnp.float32)
    for piece in pieces:
        total = total + piece.astype(jnp.float32)
    return total


def grad_kernel(scale, parts, side_ref, *refs):
    lefts, rights = refs[:parts], refs[parts:-4]
    mine, other, whole, sems = refs[-4:]
    right = jnp.concatenate([r[...] for r in rights], axis=0)
    depth = whole.shape[0]
    step = 5 * LANES
    for at in range(0, depth, step):
        end = min(at + step, depth)
        left = jnp.concatenate([l[:, at:end] for l in lefts], axis=0)
        block = lax.dot_general(
            left, right, (((0,), (0,)), ((), ())), preferred_element_type=jnp.float32
        )
        whole[at:end, :] = (block * scale).astype(jnp.bfloat16)
    half = depth // 2
    side = side_ref[0]
    copies = (
        pltpu.make_async_copy(
            whole.at[pl.ds(pl.multiple_of((1 - side) * half, 16), half)], other, sems.at[0]
        ),
        pltpu.make_async_copy(
            whole.at[pl.ds(pl.multiple_of(side * half, 16), half)], mine, sems.at[1]
        ),
    )
    for copy in copies:
        copy.start()
    for copy in copies:
        copy.wait()


def grad_halves(lefts, rights, scale):
    depth, units = lefts[0].shape[1], rights[0].shape[1]
    tokens = sum(l.shape[0] for l in lefts)
    half = jax.ShapeDtypeStruct((depth // 2, units), jnp.bfloat16)
    vmem = pl.BlockSpec(memory_space=pltpu.VMEM)
    return pl.pallas_call(
        functools.partial(grad_kernel, scale, len(lefts)),
        out_shape=(half, half),
        in_specs=[pl.BlockSpec(memory_space=pltpu.SMEM)] + [vmem] * (len(lefts) + len(rights)),
        out_specs=(pl.BlockSpec(memory_space=pl.ANY),) * 2,
        scratch_shapes=[
            pltpu.VMEM((depth, units), jnp.bfloat16),
            pltpu.SemaphoreType.DMA((2,)),
        ],
        compiler_params=pltpu.CompilerParams(vmem_limit_bytes=24 << 20),
        cost_estimate=pl.CostEstimate(
            flops=2 * depth * units * tokens, bytes_accessed=8 << 20, transcendentals=0
        ),
    )(lax.axis_index("group")[None], *lefts, *rights)


def over_cores(mine, other):
    got = to_shifted(other, "group", 1)
    return (mine.astype(jnp.float32) + got.astype(jnp.float32)).astype(jnp.bfloat16)


def z_then_x(mine, other):
    half = over_cores(mine, other)
    half = sum_shares(half, "dp_0", 0).astype(jnp.bfloat16)
    return sum_shares(half, "dp_1", 0)


def x_then_z(mine, other):
    half = over_cores(mine, other)
    rows = half.shape[0] // 8
    me = lax.axis_index("dp_1")

    def share(s):
        at = (me + s) % 4
        return jnp.concatenate(
            [
                lax.dynamic_slice_in_dim(half, (z * 4 + at) * rows, rows, axis=0)
                for z in range(2)
            ],
            axis=0,
        )

    got = [to_shifted(share(s), "dp_1", s) for s in (2, 1, 3)]
    return sum_shares(added(share(0), got).astype(jnp.bfloat16), "dp_0", 0)


def sum_over_all(value):
    devices = lax.axis_size(GROUP_DP_MP)
    parts = lax.all_to_all(
        jnp.full((devices, LANES), value, jnp.float32), GROUP_DP_MP, 0, 0, tiled=True
    )
    return jnp.sum(parts[:, 0])


def gelu_parts(pre_act):
    tangent = jnp.tanh(GELU_COEF * (pre_act + GELU_CUBE * pre_act * pre_act * pre_act))
    activation = 0.5 * pre_act * (1.0 + tangent)
    gelu_slope = 0.5 * (1.0 + tangent) + 0.5 * pre_act * (1.0 - tangent * tangent) * GELU_COEF * (
        1.0 + 3.0 * GELU_CUBE * pre_act * pre_act
    )
    return (activation, gelu_slope)


def step_factors(start_step, advantages, behaviour_gap, modulation, step_num):
    step_len = 1.0 / SCHED
    vel_coef = 1.0 + 0.5 * NOISE_SLOPE * NOISE_SLOPE
    sched_index = start_step + step_num
    time_now = 1.0 - sched_index.astype(jnp.float32) / SCHED
    onehot = (sched_index[:, None] == jnp.arange(SCHED, dtype=jnp.int32)[None, :]).astype(
        jnp.float32
    )
    mod_rows = jnp.einsum("is,scd->icd", onehot, modulation, precision=HIGH_PREC)
    noise_level = NOISE_SLOPE * jnp.sqrt(time_now / (1.0 - time_now))
    drift_x = 0.5 * NOISE_SLOPE * NOISE_SLOPE / (1.0 - time_now)
    policy_ratio = jnp.exp(behaviour_gap[:, step_num])
    active = (advantages >= 0.0) & (policy_ratio <= 1.0 + CLIP_RANGE) | (advantages < 0.0) & (
        policy_ratio >= 1.0 - CLIP_RANGE
    )
    pg_coef = jnp.where(active, policy_ratio * advantages, jnp.zeros_like(advantages))
    return (
        mod_rows[0],
        (1.0 - step_len * drift_x)[0],
        step_len * vel_coef,
        (noise_level * math.sqrt(step_len))[0],
        (pg_coef * vel_coef * math.sqrt(step_len) / noise_level)[0],
        (vel_coef * vel_coef * step_len / (noise_level * noise_level))[0],
    )


def inputs_of(latent, mod_rows):
    normed = latent * lax.rsqrt(jnp.mean(latent * latent, axis=1, keepdims=True) + 1e-06)
    return (normed * (1.0 + mod_rows[1]) + mod_rows[0]).astype(jnp.bfloat16)


def forward(inputs, w_in, w_down):
    pre_act = jnp.dot(inputs, w_in, preferred_element_type=jnp.float32) / math.sqrt(
        w_in.shape[0]
    )
    hidden = gelu_parts(pre_act)[0].astype(jnp.bfloat16)
    hidden_width = w_in.shape[1] * lax.axis_size(MP)
    partial = jnp.einsum(
        "lf,df->ld", hidden, w_down, preferred_element_type=jnp.float32
    ) / math.sqrt(hidden_width)
    return pre_act, hidden, partial.astype(jnp.bfloat16)


def next_latent(latent, velocity, noise, factors):
    _, keep, pull, spread, _, _ = factors
    step_mean = latent * keep - pull * velocity.astype(jnp.float32)
    return step_mean + spread * noise.astype(jnp.float32)


def velocity_grad(velocity, noise, ref_velocity, factors):
    gap = velocity.astype(jnp.float32) - ref_velocity.astype(jnp.float32)
    return (factors[4] * noise.astype(jnp.float32) + factors[5] * gap).astype(jnp.bfloat16)


def hidden_grad(vel_grad, w_down, pre_act, hidden_width):
    wide = jnp.einsum(
        "ld,df->lf", vel_grad, w_down, preferred_element_type=jnp.float32
    ) / math.sqrt(hidden_width)
    return (wide * gelu_parts(pre_act)[1]).astype(jnp.bfloat16)


def on_device(
    latents, noise, ref_velocity, start_step, advantages, behaviour_gap, modulation, w_in, w_down
):
    model_width = latents.shape[2]
    hidden_width = w_in.shape[1] * lax.axis_size(MP)
    block = latents.shape[1] // len(ORDER)
    early = 3 * block
    first, second = (
        step_factors(start_step, advantages, behaviour_gap, modulation, k) for k in range(2)
    )
    w_in_full, w_down_full = gathered_weights(w_in, w_down)
    x0 = to_relative(latents[0], "mp_0", 0)
    noise_0, noise_1 = (to_relative(noise[0, k], "mp_0", 0) for k in range(2))
    ref_0, ref_1 = (to_relative(ref_velocity[0, k], "mp_0", 0) for k in range(2))
    x0, noise_0, noise_1, ref_0, ref_1 = lax.optimization_barrier(
        (x0, noise_0, noise_1, ref_0, ref_1)
    )

    u_0 = inputs_of(x0, first[0])
    pre_0, hidden_0, part_0 = forward(u_0, w_in_full, w_down_full)
    got = [
        to_shifted(part_0[p * block : (p + 1) * block], "mp_0", s)
        for p, s in ((3, 2), (1, 3), (2, 1))
    ]
    rows = over_z(added(part_0[:block], got))
    v_1, v_3, v_2 = (to_shifted(rows, "mp_0", s) for s in (1, 3, 2))

    v_early = jnp.concatenate([rows, v_1, v_3], axis=0)
    x1_early = next_latent(x0[:early], v_early, noise_0[:early], first)
    u1_early = inputs_of(x1_early, second[0])
    pre1_early, hidden1_early, part_early = forward(u1_early, w_in_full, w_down_full)
    back_1 = to_shifted(part_early[block : 2 * block], "mp_0", 3)
    back_3 = to_shifted(part_early[2 * block :], "mp_0", 1)
    x1_late = next_latent(x0[early:], v_2, noise_0[early:], first)
    u1_late = inputs_of(x1_late, second[0])
    pre1_late, hidden1_late, part_late = forward(u1_late, w_in_full, w_down_full)
    back_2 = to_shifted(part_late, "mp_0", 2)

    velocity_0 = jnp.concatenate([v_early, v_2], axis=0)
    e_0 = velocity_grad(velocity_0, noise_0, ref_0, first)
    e_0 = lax.optimization_barrier(e_0)
    d_0 = hidden_grad(e_0, w_down_full, pre_0, hidden_width)
    g_0, g1_early, g1_late = lax.optimization_barrier((hidden_0, hidden1_early, hidden1_late))
    mine = added(part_early[:block], [back_1, back_3, back_2])
    mine, e_0, d_0, g_0, g1_early, g1_late = lax.optimization_barrier(
        (mine, e_0, d_0, g_0, g1_early, g1_late)
    )
    rows = over_z(mine)
    v_1, v_3, v_2 = (to_shifted(rows, "mp_0", s) for s in (1, 3, 2))
    velocity_1 = jnp.concatenate([rows, v_1, v_3, v_2], axis=0)
    e_1 = velocity_grad(velocity_1, noise_1, ref_1, second)
    e_1 = lax.optimization_barrier(e_1)
    pre_1 = jnp.concatenate([pre1_early, pre1_late], axis=0)
    g_1 = jnp.concatenate([g1_early, g1_late], axis=0)
    down_halves = grad_halves((e_0, e_1), (g_0, g_1), 1.0 / math.sqrt(hidden_width))
    d_1 = hidden_grad(e_1, w_down_full, pre_1, hidden_width)
    d_1, down_halves = lax.optimization_barrier((d_1, down_halves))
    in_halves = grad_halves(
        (u_0, u1_early, u1_late),
        (d_0, d_1),
        1.0 / math.sqrt(model_width),
    )
    down_mine = x_then_z(*down_halves)
    in_mine = z_then_x(*in_halves)
    x1 = jnp.concatenate([x1_early, x1_late], axis=0)
    x2 = next_latent(x1, velocity_1, noise_1, second)
    final = to_absolute(x2, "mp_0", 0)[None]
    total = sum_over_all(jnp.sum(in_mine * in_mine) + jnp.sum(down_mine * down_mine))
    grad_rms = jnp.sqrt(total / (2.0 * model_width * hidden_width) + 1e-06)
    new_in = (w_in.astype(jnp.float32) - in_mine / grad_rms).astype(jnp.bfloat16)
    new_down = (w_down.astype(jnp.float32) - down_mine / grad_rms).astype(jnp.bfloat16)
    return (final, new_in, new_down)


def solution(mesh):
    finer = Mesh(
        mesh.devices.reshape(mesh.shape["group"], 2, 4, 4, 4),
        ("group", "dp_0", "dp_1", "mp_0", "mp_1"),
    )
    placed = (
        P(GROUP_DP, None, None),
        P(GROUP_DP, None, None, None),
        P(GROUP_DP, None, None, None),
        P(GROUP_DP),
        P(GROUP_DP),
        P(GROUP_DP, None),
        P(),
        P(GROUP_DP, MP),
        P(GROUP_DP, MP),
    )
    return jax.shard_map(
        on_device,
        mesh=finer,
        in_specs=placed,
        out_specs=(P(GROUP_DP, None, None), P(GROUP_DP, MP), P(GROUP_DP, MP)),
        check_vma=False,
    )
```

```python
import functools
import math

import jax
import jax.numpy as jnp
from jax import lax
from jax.experimental import pallas as pl
from jax.experimental.pallas import tpu as pltpu
from jax.sharding import Mesh
from jax.sharding import PartitionSpec as P

SCHED = 10
MP = ("mp_0", "mp_1")
GROUP_DP = ("group", "dp_0", "dp_1")
GROUP_DP_MP = ("group", "dp_0", "dp_1", "mp_0", "mp_1")


NOISE_SLOPE = 0.7
CLIP_RANGE = 0.2
GELU_COEF = 0.7978845608028654
GELU_CUBE = 0.044715
HIGH_PREC = lax.Precision.HIGHEST


def to_shifted(array, axis, shift):
    peers = lax.axis_size(axis)
    return lax.ppermute(array, axis, [(i, (i + shift) % peers) for i in range(peers)])


def share_for(array, axis, shift, dim):
    peers = lax.axis_size(axis)
    length = array.shape[dim] // peers
    at = (lax.axis_index(axis) + shift) % peers
    return lax.dynamic_slice_in_dim(array, at * length, length, axis=dim)


def sum_shares(array, axis, dim):
    peers = lax.axis_size(axis)
    got = [
        to_shifted(share_for(array, axis, s, dim), axis, s)
        for s in sorted(range(1, peers), key=lambda s: -min(s, peers - s))
    ]
    total = share_for(array, axis, 0, dim).astype(jnp.float32)
    for piece in got:
        total = total + piece.astype(jnp.float32)
    return total


def join_shares(share, axis, dim):
    peers = lax.axis_size(axis)
    me = lax.axis_index(axis)
    if peers == 2:
        other = to_shifted(share, axis, 1)
        first = me == 0
        return jnp.concatenate(
            [jnp.where(first, share, other), jnp.where(first, other, share)], axis=dim
        )
    length = share.shape[dim]
    shifts = sorted(range(1, peers), key=lambda s: -min(s, peers - s))
    got = [to_shifted(share, axis, s) for s in shifts]
    shape = list(share.shape)
    shape[dim] = length * peers
    whole = jnp.zeros(shape, share.dtype)
    for s, piece in zip([0] + shifts, [share] + got):
        at = (me - s) % peers
        whole = lax.dynamic_update_slice_in_dim(whole, piece, at * length, axis=dim)
    return whole


def gathered_weights(w_in, w_down):
    rows, units = w_in.shape
    in_x = join_shares(w_in, "dp_1", 0)
    down_z = join_shares(w_down[None], "dp_0", 0)
    in_xz = join_shares(in_x, "dp_0", 0)
    down_zx = join_shares(down_z[:, None], "dp_1", 1)
    w_in_full = join_shares(in_xz, "group", 0)
    w_down_full = join_shares(down_zx.reshape(-1, units), "group", 0)
    return (w_in_full, w_down_full)


LANES = 128


def picked(pieces, me, c):
    r = (me - c) % len(pieces)
    out = pieces[-1]
    for k in range(len(pieces) - 2, -1, -1):
        out = jnp.where(r == k, pieces[k], out)
    return out


def over_z(mine):
    width = mine.shape[1]
    peers = lax.axis_size("mp_1")
    spare = -width % (peers * LANES)
    mine = jnp.pad(mine, ((0, 0), (0, spare))).astype(jnp.bfloat16)
    piece = sum_shares(mine, "mp_1", 1).astype(jnp.bfloat16)
    pieces = [piece] + [to_shifted(piece, "mp_1", s) for s in (1, 2, 3)]
    me = lax.axis_index("mp_1")
    rows = jnp.concatenate([picked(pieces, me, c) for c in range(peers)], axis=1)
    return rows[:, :width]


def over_y(partial):
    return sum_shares(partial, "mp_0", 0)


def added(own, pieces):
    total = own.astype(jnp.float32)
    for piece in pieces:
        total = total + piece.astype(jnp.float32)
    return total


def grad_kernel(scale, parts, side_ref, *refs):
    lefts, rights = refs[:parts], refs[parts:-4]
    mine, other, whole, sems = refs[-4:]
    right = jnp.concatenate([r[...] for r in rights], axis=0)
    depth = whole.shape[0]
    step = 5 * LANES
    for at in range(0, depth, step):
        end = min(at + step, depth)
        left = jnp.concatenate([l[:, at:end] for l in lefts], axis=0)
        block = lax.dot_general(
            left, right, (((0,), (0,)), ((), ())), preferred_element_type=jnp.float32
        )
        whole[at:end, :] = (block * scale).astype(jnp.bfloat16)
    half = depth // 2
    side = side_ref[0]
    copies = (
        pltpu.make_async_copy(
            whole.at[pl.ds(pl.multiple_of((1 - side) * half, 16), half)], other, sems.at[0]
        ),
        pltpu.make_async_copy(
            whole.at[pl.ds(pl.multiple_of(side * half, 16), half)], mine, sems.at[1]
        ),
    )
    for copy in copies:
        copy.start()
    for copy in copies:
        copy.wait()


def grad_halves(lefts, rights, scale):
    depth, units = lefts[0].shape[1], rights[0].shape[1]
    tokens = sum(l.shape[0] for l in lefts)
    half = jax.ShapeDtypeStruct((depth // 2, units), jnp.bfloat16)
    vmem = pl.BlockSpec(memory_space=pltpu.VMEM)
    return pl.pallas_call(
        functools.partial(grad_kernel, scale, len(lefts)),
        out_shape=(half, half),
        in_specs=[pl.BlockSpec(memory_space=pltpu.SMEM)] + [vmem] * (len(lefts) + len(rights)),
        out_specs=(pl.BlockSpec(memory_space=pl.ANY),) * 2,
        scratch_shapes=[
            pltpu.VMEM((depth, units), jnp.bfloat16),
            pltpu.SemaphoreType.DMA((2,)),
        ],
        compiler_params=pltpu.CompilerParams(vmem_limit_bytes=24 << 20),
        cost_estimate=pl.CostEstimate(
            flops=2 * depth * units * tokens, bytes_accessed=8 << 20, transcendentals=0
        ),
    )(lax.axis_index("group")[None], *lefts, *rights)


def over_cores(mine, other):
    got = to_shifted(other, "group", 1)
    return (mine.astype(jnp.float32) + got.astype(jnp.float32)).astype(jnp.bfloat16)


def z_then_x(half):
    half = sum_shares(half, "dp_0", 0).astype(jnp.bfloat16)
    return sum_shares(half, "dp_1", 0)


def x_then_z(half):
    rows = half.shape[0] // 8
    me = lax.axis_index("dp_1")

    def share(s):
        at = (me + s) % 4
        return jnp.concatenate(
            [
                lax.dynamic_slice_in_dim(half, (z * 4 + at) * rows, rows, axis=0)
                for z in range(2)
            ],
            axis=0,
        )

    got = [to_shifted(share(s), "dp_1", s) for s in (2, 1, 3)]
    return sum_shares(added(share(0), got).astype(jnp.bfloat16), "dp_0", 0)


def sum_over_all(value):
    devices = lax.axis_size(GROUP_DP_MP)
    parts = lax.all_to_all(
        jnp.full((devices, LANES), value, jnp.float32), GROUP_DP_MP, 0, 0, tiled=True
    )
    return jnp.sum(parts[:, 0])


def gelu_parts(pre_act):
    tangent = jnp.tanh(GELU_COEF * (pre_act + GELU_CUBE * pre_act * pre_act * pre_act))
    activation = 0.5 * pre_act * (1.0 + tangent)
    gelu_slope = 0.5 * (1.0 + tangent) + 0.5 * pre_act * (1.0 - tangent * tangent) * GELU_COEF * (
        1.0 + 3.0 * GELU_CUBE * pre_act * pre_act
    )
    return (activation, gelu_slope)


def step_factors(start_step, advantages, behaviour_gap, modulation, step_num):
    step_len = 1.0 / SCHED
    vel_coef = 1.0 + 0.5 * NOISE_SLOPE * NOISE_SLOPE
    sched_index = start_step + step_num
    time_now = 1.0 - sched_index.astype(jnp.float32) / SCHED
    onehot = (sched_index[:, None] == jnp.arange(SCHED, dtype=jnp.int32)[None, :]).astype(
        jnp.float32
    )
    mod_rows = jnp.einsum("is,scd->icd", onehot, modulation, precision=HIGH_PREC)
    noise_level = NOISE_SLOPE * jnp.sqrt(time_now / (1.0 - time_now))
    drift_x = 0.5 * NOISE_SLOPE * NOISE_SLOPE / (1.0 - time_now)
    policy_ratio = jnp.exp(behaviour_gap[:, step_num])
    active = (advantages >= 0.0) & (policy_ratio <= 1.0 + CLIP_RANGE) | (advantages < 0.0) & (
        policy_ratio >= 1.0 - CLIP_RANGE
    )
    pg_coef = jnp.where(active, policy_ratio * advantages, jnp.zeros_like(advantages))
    return (
        mod_rows[0],
        (1.0 - step_len * drift_x)[0],
        step_len * vel_coef,
        (noise_level * math.sqrt(step_len))[0],
        (pg_coef * vel_coef * math.sqrt(step_len) / noise_level)[0],
        (vel_coef * vel_coef * step_len / (noise_level * noise_level))[0],
    )


def inputs_of(latent, mod_rows):
    normed = latent * lax.rsqrt(jnp.mean(latent * latent, axis=1, keepdims=True) + 1e-06)
    return (normed * (1.0 + mod_rows[1]) + mod_rows[0]).astype(jnp.bfloat16)


def forward(inputs, w_in, w_down):
    pre_act = jnp.dot(inputs, w_in, preferred_element_type=jnp.float32) / math.sqrt(
        w_in.shape[0]
    )
    hidden = gelu_parts(pre_act)[0].astype(jnp.bfloat16)
    hidden_width = w_in.shape[1] * lax.axis_size(MP)
    partial = jnp.einsum(
        "lf,df->ld", hidden, w_down, preferred_element_type=jnp.float32
    ) / math.sqrt(hidden_width)
    return pre_act, hidden, partial.astype(jnp.bfloat16)


def next_latent(latent, velocity, noise, factors):
    _, keep, pull, spread, _, _ = factors
    step_mean = latent * keep - pull * velocity.astype(jnp.float32)
    return step_mean + spread * noise.astype(jnp.float32)


def velocity_grad(velocity, noise, ref_velocity, factors):
    gap = velocity.astype(jnp.float32) - ref_velocity.astype(jnp.float32)
    return (factors[4] * noise.astype(jnp.float32) + factors[5] * gap).astype(jnp.bfloat16)


def hidden_grad(vel_grad, w_down, pre_act, hidden_width):
    wide = jnp.einsum(
        "ld,df->lf", vel_grad, w_down, preferred_element_type=jnp.float32
    ) / math.sqrt(hidden_width)
    return (wide * gelu_parts(pre_act)[1]).astype(jnp.bfloat16)


def on_device(
    latents, noise, ref_velocity, start_step, advantages, behaviour_gap, modulation, w_in, w_down
):
    model_width = latents.shape[2]
    hidden_width = w_in.shape[1] * lax.axis_size(MP)
    first, second = (
        step_factors(start_step, advantages, behaviour_gap, modulation, k) for k in range(2)
    )
    w_in_full, w_down_full = gathered_weights(w_in, w_down)
    u_0 = inputs_of(latents[0], first[0])
    pre_0, hidden_0, part_0 = forward(u_0, w_in_full, w_down_full)
    velocity_0 = join_shares(over_z(over_y(part_0)), "mp_0", 0)
    x1 = next_latent(latents[0], velocity_0, noise[0, 0], first)
    u_1 = inputs_of(x1, second[0])
    pre_1, hidden_1, part_1 = forward(u_1, w_in_full, w_down_full)
    part_1, velocity_b = lax.optimization_barrier((part_1, velocity_0))
    e_0 = velocity_grad(velocity_b, noise[0, 0], ref_velocity[0, 0], first)
    e_0 = lax.optimization_barrier(e_0)
    d_0 = hidden_grad(e_0, w_down_full, pre_0, hidden_width)
    g_0, g_1 = lax.optimization_barrier((hidden_0, hidden_1))
    mine, e_0, d_0, g_0, g_1 = lax.optimization_barrier((over_y(part_1), e_0, d_0, g_0, g_1))
    velocity_1 = join_shares(over_z(mine), "mp_0", 0)
    e_1 = velocity_grad(velocity_1, noise[0, 1], ref_velocity[0, 1], second)
    e_1 = lax.optimization_barrier(e_1)
    d_1 = lax.optimization_barrier(hidden_grad(e_1, w_down_full, pre_1, hidden_width))
    in_halves = grad_halves((u_0, u_1), (d_0, d_1), 1.0 / math.sqrt(model_width))
    in_halves, e_1, velocity_1 = lax.optimization_barrier((in_halves, e_1, velocity_1))
    down_halves = grad_halves((e_0, e_1), (g_0, g_1), 1.0 / math.sqrt(hidden_width))
    in_half, down_halves, velocity_1 = lax.optimization_barrier(
        (over_cores(*in_halves), down_halves, velocity_1)
    )
    in_mine = z_then_x(in_half)
    down_mine = x_then_z(over_cores(*down_halves))
    final = next_latent(x1, velocity_1, noise[0, 1], second)[None]
    total = sum_over_all(jnp.sum(in_mine * in_mine) + jnp.sum(down_mine * down_mine))
    grad_rms = jnp.sqrt(total / (2.0 * model_width * hidden_width) + 1e-06)
    new_in = (w_in.astype(jnp.float32) - in_mine / grad_rms).astype(jnp.bfloat16)
    new_down = (w_down.astype(jnp.float32) - down_mine / grad_rms).astype(jnp.bfloat16)
    return (final, new_in, new_down)


def solution(mesh):
    finer = Mesh(
        mesh.devices.reshape(mesh.shape["group"], 2, 4, 4, 4),
        ("group", "dp_0", "dp_1", "mp_0", "mp_1"),
    )
    placed = (
        P(GROUP_DP, None, None),
        P(GROUP_DP, None, None, None),
        P(GROUP_DP, None, None, None),
        P(GROUP_DP),
        P(GROUP_DP),
        P(GROUP_DP, None),
        P(),
        P(GROUP_DP, MP),
        P(GROUP_DP, MP),
    )
    return jax.shard_map(
        on_device,
        mesh=finer,
        in_specs=placed,
        out_specs=(P(GROUP_DP, None, None), P(GROUP_DP, MP), P(GROUP_DP, MP)),
        check_vma=False,
    )
```

```python
import functools
import math

import jax
import jax.numpy as jnp
from jax import lax
from jax.experimental import pallas as pl
from jax.experimental.pallas import tpu as pltpu
from jax.sharding import Mesh
from jax.sharding import PartitionSpec as P

SCHED = 10
MP = ("mp_0", "mp_1")
GROUP_DP = ("group", "dp_0", "dp_1")
GROUP_DP_MP = ("group", "dp_0", "dp_1", "mp_0", "mp_1")


NOISE_SLOPE = 0.7
CLIP_RANGE = 0.2
GELU_COEF = 0.7978845608028654
GELU_CUBE = 0.044715
HIGH_PREC = lax.Precision.HIGHEST


def to_shifted(array, axis, shift):
    peers = lax.axis_size(axis)
    return lax.ppermute(array, axis, [(i, (i + shift) % peers) for i in range(peers)])


def share_for(array, axis, shift, dim):
    peers = lax.axis_size(axis)
    length = array.shape[dim] // peers
    at = (lax.axis_index(axis) + shift) % peers
    return lax.dynamic_slice_in_dim(array, at * length, length, axis=dim)


def sum_shares(array, axis, dim):
    peers = lax.axis_size(axis)
    got = [
        to_shifted(share_for(array, axis, s, dim), axis, s)
        for s in sorted(range(1, peers), key=lambda s: -min(s, peers - s))
    ]
    total = share_for(array, axis, 0, dim).astype(jnp.float32)
    for piece in got:
        total = total + piece.astype(jnp.float32)
    return total


def join_shares(share, axis, dim):
    peers = lax.axis_size(axis)
    me = lax.axis_index(axis)
    if peers == 2:
        other = to_shifted(share, axis, 1)
        first = me == 0
        return jnp.concatenate(
            [jnp.where(first, share, other), jnp.where(first, other, share)], axis=dim
        )
    length = share.shape[dim]
    shifts = sorted(range(1, peers), key=lambda s: -min(s, peers - s))
    got = [to_shifted(share, axis, s) for s in shifts]
    shape = list(share.shape)
    shape[dim] = length * peers
    whole = jnp.zeros(shape, share.dtype)
    for s, piece in zip([0] + shifts, [share] + got):
        at = (me - s) % peers
        whole = lax.dynamic_update_slice_in_dim(whole, piece, at * length, axis=dim)
    return whole


def gathered_weights(w_in, w_down):
    rows, units = w_in.shape
    in_x = join_shares(w_in, "dp_1", 0)
    down_z = join_shares(w_down[None], "dp_0", 0)
    in_xz = join_shares(in_x, "dp_0", 0)
    down_zx = join_shares(down_z[:, None], "dp_1", 1)
    w_in_full = join_shares(in_xz, "group", 0)
    w_down_full = join_shares(down_zx.reshape(-1, units), "group", 0)
    return (w_in_full, w_down_full)


LANES = 128


def picked(pieces, me, c):
    r = (me - c) % len(pieces)
    out = pieces[-1]
    for k in range(len(pieces) - 2, -1, -1):
        out = jnp.where(r == k, pieces[k], out)
    return out


def over_z(mine):
    width = mine.shape[1]
    peers = lax.axis_size("mp_1")
    spare = -width % (peers * LANES)
    mine = jnp.pad(mine, ((0, 0), (0, spare))).astype(jnp.bfloat16)
    piece = sum_shares(mine, "mp_1", 1).astype(jnp.bfloat16)
    pieces = [piece] + [to_shifted(piece, "mp_1", s) for s in (1, 2, 3)]
    me = lax.axis_index("mp_1")
    rows = jnp.concatenate([picked(pieces, me, c) for c in range(peers)], axis=1)
    return rows[:, :width]


def over_y(partial):
    return sum_shares(partial, "mp_0", 0)


def added(own, pieces):
    total = own.astype(jnp.float32)
    for piece in pieces:
        total = total + piece.astype(jnp.float32)
    return total


def grad_kernel(scale, parts, side_ref, *refs):
    lefts, rights = refs[:parts], refs[parts:-4]
    mine, other, whole, sems = refs[-4:]
    right = jnp.concatenate([r[...] for r in rights], axis=0)
    depth = whole.shape[0]
    step = 5 * LANES
    for at in range(0, depth, step):
        end = min(at + step, depth)
        left = jnp.concatenate([l[:, at:end] for l in lefts], axis=0)
        block = lax.dot_general(
            left, right, (((0,), (0,)), ((), ())), preferred_element_type=jnp.float32
        )
        whole[at:end, :] = (block * scale).astype(jnp.bfloat16)
    half = depth // 2
    side = side_ref[0]
    copies = (
        pltpu.make_async_copy(
            whole.at[pl.ds(pl.multiple_of((1 - side) * half, 16), half)], other, sems.at[0]
        ),
        pltpu.make_async_copy(
            whole.at[pl.ds(pl.multiple_of(side * half, 16), half)], mine, sems.at[1]
        ),
    )
    for copy in copies:
        copy.start()
    for copy in copies:
        copy.wait()


def grad_halves(lefts, rights, scale):
    depth, units = lefts[0].shape[1], rights[0].shape[1]
    tokens = sum(l.shape[0] for l in lefts)
    half = jax.ShapeDtypeStruct((depth // 2, units), jnp.bfloat16)
    vmem = pl.BlockSpec(memory_space=pltpu.VMEM)
    return pl.pallas_call(
        functools.partial(grad_kernel, scale, len(lefts)),
        out_shape=(half, half),
        in_specs=[pl.BlockSpec(memory_space=pltpu.SMEM)] + [vmem] * (len(lefts) + len(rights)),
        out_specs=(pl.BlockSpec(memory_space=pl.ANY),) * 2,
        scratch_shapes=[
            pltpu.VMEM((depth, units), jnp.bfloat16),
            pltpu.SemaphoreType.DMA((2,)),
        ],
        compiler_params=pltpu.CompilerParams(vmem_limit_bytes=24 << 20),
        cost_estimate=pl.CostEstimate(
            flops=2 * depth * units * tokens, bytes_accessed=8 << 20, transcendentals=0
        ),
    )(lax.axis_index("group")[None], *lefts, *rights)


def over_cores(mine, other):
    got = to_shifted(other, "group", 1)
    return (mine.astype(jnp.float32) + got.astype(jnp.float32)).astype(jnp.bfloat16)


def z_then_x(half):
    half = sum_shares(half, "dp_0", 0).astype(jnp.bfloat16)
    return sum_shares(half, "dp_1", 0)


def x_then_z(half):
    rows = half.shape[0] // 8
    me = lax.axis_index("dp_1")

    def share(s):
        at = (me + s) % 4
        return jnp.concatenate(
            [
                lax.dynamic_slice_in_dim(half, (z * 4 + at) * rows, rows, axis=0)
                for z in range(2)
            ],
            axis=0,
        )

    got = [to_shifted(share(s), "dp_1", s) for s in (2, 1, 3)]
    return sum_shares(added(share(0), got).astype(jnp.bfloat16), "dp_0", 0)


def sum_over_all(value):
    devices = lax.axis_size(GROUP_DP_MP)
    parts = lax.all_to_all(
        jnp.full((devices, LANES), value, jnp.float32), GROUP_DP_MP, 0, 0, tiled=True
    )
    return jnp.sum(parts[:, 0])


def gelu_parts(pre_act):
    tangent = jnp.tanh(GELU_COEF * (pre_act + GELU_CUBE * pre_act * pre_act * pre_act))
    activation = 0.5 * pre_act * (1.0 + tangent)
    gelu_slope = 0.5 * (1.0 + tangent) + 0.5 * pre_act * (1.0 - tangent * tangent) * GELU_COEF * (
        1.0 + 3.0 * GELU_CUBE * pre_act * pre_act
    )
    return (activation, gelu_slope)


def step_factors(start_step, advantages, behaviour_gap, modulation, step_num):
    step_len = 1.0 / SCHED
    vel_coef = 1.0 + 0.5 * NOISE_SLOPE * NOISE_SLOPE
    sched_index = start_step + step_num
    time_now = 1.0 - sched_index.astype(jnp.float32) / SCHED
    onehot = (sched_index[:, None] == jnp.arange(SCHED, dtype=jnp.int32)[None, :]).astype(
        jnp.float32
    )
    mod_rows = jnp.einsum("is,scd->icd", onehot, modulation, precision=HIGH_PREC)
    noise_level = NOISE_SLOPE * jnp.sqrt(time_now / (1.0 - time_now))
    drift_x = 0.5 * NOISE_SLOPE * NOISE_SLOPE / (1.0 - time_now)
    policy_ratio = jnp.exp(behaviour_gap[:, step_num])
    active = (advantages >= 0.0) & (policy_ratio <= 1.0 + CLIP_RANGE) | (advantages < 0.0) & (
        policy_ratio >= 1.0 - CLIP_RANGE
    )
    pg_coef = jnp.where(active, policy_ratio * advantages, jnp.zeros_like(advantages))
    return (
        mod_rows[0],
        (1.0 - step_len * drift_x)[0],
        step_len * vel_coef,
        (noise_level * math.sqrt(step_len))[0],
        (pg_coef * vel_coef * math.sqrt(step_len) / noise_level)[0],
        (vel_coef * vel_coef * step_len / (noise_level * noise_level))[0],
    )


def inputs_of(latent, mod_rows):
    normed = latent * lax.rsqrt(jnp.mean(latent * latent, axis=1, keepdims=True) + 1e-06)
    return (normed * (1.0 + mod_rows[1]) + mod_rows[0]).astype(jnp.bfloat16)


def forward(inputs, w_in, w_down):
    pre_act = jnp.dot(inputs, w_in, preferred_element_type=jnp.float32) / math.sqrt(
        w_in.shape[0]
    )
    hidden = gelu_parts(pre_act)[0].astype(jnp.bfloat16)
    hidden_width = w_in.shape[1] * lax.axis_size(MP)
    partial = jnp.einsum(
        "lf,df->ld", hidden, w_down, preferred_element_type=jnp.float32
    ) / math.sqrt(hidden_width)
    return pre_act, hidden, partial.astype(jnp.bfloat16)


def next_latent(latent, velocity, noise, factors):
    _, keep, pull, spread, _, _ = factors
    step_mean = latent * keep - pull * velocity.astype(jnp.float32)
    return step_mean + spread * noise.astype(jnp.float32)


def velocity_grad(velocity, noise, ref_velocity, factors):
    gap = velocity.astype(jnp.float32) - ref_velocity.astype(jnp.float32)
    return (factors[4] * noise.astype(jnp.float32) + factors[5] * gap).astype(jnp.bfloat16)


def hidden_grad(vel_grad, w_down, pre_act, hidden_width):
    wide = jnp.einsum(
        "ld,df->lf", vel_grad, w_down, preferred_element_type=jnp.float32
    ) / math.sqrt(hidden_width)
    return (wide * gelu_parts(pre_act)[1]).astype(jnp.bfloat16)


def on_device(
    latents, noise, ref_velocity, start_step, advantages, behaviour_gap, modulation, w_in, w_down
):
    model_width = latents.shape[2]
    hidden_width = w_in.shape[1] * lax.axis_size(MP)
    first, second = (
        step_factors(start_step, advantages, behaviour_gap, modulation, k) for k in range(2)
    )
    w_in_full, w_down_full = gathered_weights(w_in, w_down)
    u_0 = inputs_of(latents[0], first[0])
    pre_0, hidden_0, part_0 = forward(u_0, w_in_full, w_down_full)
    velocity_0 = join_shares(over_z(over_y(part_0)), "mp_0", 0)
    x1 = next_latent(latents[0], velocity_0, noise[0, 0], first)
    u_1 = inputs_of(x1, second[0])
    pre_1, hidden_1, part_1 = forward(u_1, w_in_full, w_down_full)
    mine, velocity_b = lax.optimization_barrier((over_y(part_1), velocity_0))
    e_0 = velocity_grad(velocity_b, noise[0, 0], ref_velocity[0, 0], first)
    e_0 = lax.optimization_barrier(e_0)
    d_0 = hidden_grad(e_0, w_down_full, pre_0, hidden_width)
    g_0, g_1 = lax.optimization_barrier((hidden_0, hidden_1))
    rows, e_0, d_0, g_0, g_1 = lax.optimization_barrier((over_z(mine), e_0, d_0, g_0, g_1))
    velocity_1 = join_shares(rows, "mp_0", 0)
    e_1 = velocity_grad(velocity_1, noise[0, 1], ref_velocity[0, 1], second)
    e_1 = lax.optimization_barrier(e_1)
    d_1 = lax.optimization_barrier(hidden_grad(e_1, w_down_full, pre_1, hidden_width))
    in_halves = grad_halves((u_0, u_1), (d_0, d_1), 1.0 / math.sqrt(model_width))
    in_halves, e_1, velocity_1 = lax.optimization_barrier((in_halves, e_1, velocity_1))
    down_own, down_other = grad_halves((e_0, e_1), (g_0, g_1), 1.0 / math.sqrt(hidden_width))
    in_half, down_own, velocity_1 = lax.optimization_barrier(
        (over_cores(*in_halves), down_own, velocity_1)
    )
    in_mine = z_then_x(in_half)
    down_mine = x_then_z(over_cores(down_own, down_other))
    final = next_latent(x1, velocity_1, noise[0, 1], second)[None]
    total = sum_over_all(jnp.sum(in_mine * in_mine) + jnp.sum(down_mine * down_mine))
    grad_rms = jnp.sqrt(total / (2.0 * model_width * hidden_width) + 1e-06)
    new_in = (w_in.astype(jnp.float32) - in_mine / grad_rms).astype(jnp.bfloat16)
    new_down = (w_down.astype(jnp.float32) - down_mine / grad_rms).astype(jnp.bfloat16)
    return (final, new_in, new_down)


def solution(mesh):
    finer = Mesh(
        mesh.devices.reshape(mesh.shape["group"], 2, 4, 4, 4),
        ("group", "dp_0", "dp_1", "mp_0", "mp_1"),
    )
    placed = (
        P(GROUP_DP, None, None),
        P(GROUP_DP, None, None, None),
        P(GROUP_DP, None, None, None),
        P(GROUP_DP),
        P(GROUP_DP),
        P(GROUP_DP, None),
        P(),
        P(GROUP_DP, MP),
        P(GROUP_DP, MP),
    )
    return jax.shard_map(
        on_device,
        mesh=finer,
        in_specs=placed,
        out_specs=(P(GROUP_DP, None, None), P(GROUP_DP, MP), P(GROUP_DP, MP)),
        check_vma=False,
    )
```

```python
import functools
import math

import jax
import jax.numpy as jnp
from jax import lax
from jax.experimental import pallas as pl
from jax.experimental.pallas import tpu as pltpu
from jax.sharding import Mesh
from jax.sharding import PartitionSpec as P

SCHED = 10
MP = ("mp_0", "mp_1")
GROUP_DP = ("group", "dp_0", "dp_1")
GROUP_DP_MP = ("group", "dp_0", "dp_1", "mp_0", "mp_1")


NOISE_SLOPE = 0.7
CLIP_RANGE = 0.2
GELU_COEF = 0.7978845608028654
GELU_CUBE = 0.044715
HIGH_PREC = lax.Precision.HIGHEST


def to_shifted(array, axis, shift):
    peers = lax.axis_size(axis)
    return lax.ppermute(array, axis, [(i, (i + shift) % peers) for i in range(peers)])


def share_for(array, axis, shift, dim):
    peers = lax.axis_size(axis)
    length = array.shape[dim] // peers
    at = (lax.axis_index(axis) + shift) % peers
    return lax.dynamic_slice_in_dim(array, at * length, length, axis=dim)


def sum_shares(array, axis, dim):
    peers = lax.axis_size(axis)
    got = [
        to_shifted(share_for(array, axis, s, dim), axis, s)
        for s in sorted(range(1, peers), key=lambda s: -min(s, peers - s))
    ]
    total = share_for(array, axis, 0, dim).astype(jnp.float32)
    for piece in got:
        total = total + piece.astype(jnp.float32)
    return total


def join_shares(share, axis, dim):
    peers = lax.axis_size(axis)
    me = lax.axis_index(axis)
    if peers == 2:
        other = to_shifted(share, axis, 1)
        first = me == 0
        return jnp.concatenate(
            [jnp.where(first, share, other), jnp.where(first, other, share)], axis=dim
        )
    length = share.shape[dim]
    shifts = sorted(range(1, peers), key=lambda s: -min(s, peers - s))
    got = [to_shifted(share, axis, s) for s in shifts]
    shape = list(share.shape)
    shape[dim] = length * peers
    whole = jnp.zeros(shape, share.dtype)
    for s, piece in zip([0] + shifts, [share] + got):
        at = (me - s) % peers
        whole = lax.dynamic_update_slice_in_dim(whole, piece, at * length, axis=dim)
    return whole


def gathered_weights(w_in, w_down):
    rows, units = w_in.shape
    in_x = join_shares(w_in, "dp_1", 0)
    down_z = join_shares(w_down[None], "dp_0", 0)
    in_xz = join_shares(in_x, "dp_0", 0)
    down_zx = join_shares(down_z[:, None], "dp_1", 1)
    w_in_full = join_shares(in_xz, "group", 0)
    w_down_full = join_shares(down_zx.reshape(-1, units), "group", 0)
    return (w_in_full, w_down_full)


LANES = 128


def picked(pieces, me, c):
    r = (me - c) % len(pieces)
    out = pieces[-1]
    for k in range(len(pieces) - 2, -1, -1):
        out = jnp.where(r == k, pieces[k], out)
    return out


def over_z(mine):
    width = mine.shape[1]
    peers = lax.axis_size("mp_1")
    spare = -width % (peers * LANES)
    mine = jnp.pad(mine, ((0, 0), (0, spare))).astype(jnp.bfloat16)
    piece = sum_shares(mine, "mp_1", 1).astype(jnp.bfloat16)
    pieces = [piece] + [to_shifted(piece, "mp_1", s) for s in (1, 2, 3)]
    me = lax.axis_index("mp_1")
    rows = jnp.concatenate([picked(pieces, me, c) for c in range(peers)], axis=1)
    return rows[:, :width]


def over_y(partial):
    return sum_shares(partial, "mp_0", 0)


def added(own, pieces):
    total = own.astype(jnp.float32)
    for piece in pieces:
        total = total + piece.astype(jnp.float32)
    return total


def grad_kernel(scale, parts, side_ref, *refs):
    lefts, rights = refs[:parts], refs[parts:-4]
    mine, other, whole, sems = refs[-4:]
    right = jnp.concatenate([r[...] for r in rights], axis=0)
    depth = whole.shape[0]
    step = 5 * LANES
    for at in range(0, depth, step):
        end = min(at + step, depth)
        left = jnp.concatenate([l[:, at:end] for l in lefts], axis=0)
        block = lax.dot_general(
            left, right, (((0,), (0,)), ((), ())), preferred_element_type=jnp.float32
        )
        whole[at:end, :] = (block * scale).astype(jnp.bfloat16)
    half = depth // 2
    side = side_ref[0]
    copies = (
        pltpu.make_async_copy(
            whole.at[pl.ds(pl.multiple_of((1 - side) * half, 16), half)], other, sems.at[0]
        ),
        pltpu.make_async_copy(
            whole.at[pl.ds(pl.multiple_of(side * half, 16), half)], mine, sems.at[1]
        ),
    )
    for copy in copies:
        copy.start()
    for copy in copies:
        copy.wait()


def grad_halves(lefts, rights, scale):
    depth, units = lefts[0].shape[1], rights[0].shape[1]
    tokens = sum(l.shape[0] for l in lefts)
    half = jax.ShapeDtypeStruct((depth // 2, units), jnp.bfloat16)
    vmem = pl.BlockSpec(memory_space=pltpu.VMEM)
    return pl.pallas_call(
        functools.partial(grad_kernel, scale, len(lefts)),
        out_shape=(half, half),
        in_specs=[pl.BlockSpec(memory_space=pltpu.SMEM)] + [vmem] * (len(lefts) + len(rights)),
        out_specs=(pl.BlockSpec(memory_space=pl.ANY),) * 2,
        scratch_shapes=[
            pltpu.VMEM((depth, units), jnp.bfloat16),
            pltpu.SemaphoreType.DMA((2,)),
        ],
        compiler_params=pltpu.CompilerParams(vmem_limit_bytes=24 << 20),
        cost_estimate=pl.CostEstimate(
            flops=2 * depth * units * tokens, bytes_accessed=8 << 20, transcendentals=0
        ),
    )(lax.axis_index("group")[None], *lefts, *rights)


def over_cores(mine, other):
    got = to_shifted(other, "group", 1)
    return (mine.astype(jnp.float32) + got.astype(jnp.float32)).astype(jnp.bfloat16)


def z_then_x(half):
    half = sum_shares(half, "dp_0", 0).astype(jnp.bfloat16)
    return sum_shares(half, "dp_1", 0)


def x_then_z(half):
    rows = half.shape[0] // 8
    me = lax.axis_index("dp_1")

    def share(s):
        at = (me + s) % 4
        return jnp.concatenate(
            [
                lax.dynamic_slice_in_dim(half, (z * 4 + at) * rows, rows, axis=0)
                for z in range(2)
            ],
            axis=0,
        )

    got = [to_shifted(share(s), "dp_1", s) for s in (2, 1, 3)]
    return sum_shares(added(share(0), got).astype(jnp.bfloat16), "dp_0", 0)


def sum_over_all(value):
    devices = lax.axis_size(GROUP_DP_MP)
    parts = lax.all_to_all(
        jnp.full((devices, LANES), value, jnp.float32), GROUP_DP_MP, 0, 0, tiled=True
    )
    return jnp.sum(parts[:, 0])


def gelu_parts(pre_act):
    tangent = jnp.tanh(GELU_COEF * (pre_act + GELU_CUBE * pre_act * pre_act * pre_act))
    activation = 0.5 * pre_act * (1.0 + tangent)
    gelu_slope = 0.5 * (1.0 + tangent) + 0.5 * pre_act * (1.0 - tangent * tangent) * GELU_COEF * (
        1.0 + 3.0 * GELU_CUBE * pre_act * pre_act
    )
    return (activation, gelu_slope)


def step_factors(start_step, advantages, behaviour_gap, modulation, step_num):
    step_len = 1.0 / SCHED
    vel_coef = 1.0 + 0.5 * NOISE_SLOPE * NOISE_SLOPE
    sched_index = start_step + step_num
    time_now = 1.0 - sched_index.astype(jnp.float32) / SCHED
    onehot = (sched_index[:, None] == jnp.arange(SCHED, dtype=jnp.int32)[None, :]).astype(
        jnp.float32
    )
    mod_rows = jnp.einsum("is,scd->icd", onehot, modulation, precision=HIGH_PREC)
    noise_level = NOISE_SLOPE * jnp.sqrt(time_now / (1.0 - time_now))
    drift_x = 0.5 * NOISE_SLOPE * NOISE_SLOPE / (1.0 - time_now)
    policy_ratio = jnp.exp(behaviour_gap[:, step_num])
    active = (advantages >= 0.0) & (policy_ratio <= 1.0 + CLIP_RANGE) | (advantages < 0.0) & (
        policy_ratio >= 1.0 - CLIP_RANGE
    )
    pg_coef = jnp.where(active, policy_ratio * advantages, jnp.zeros_like(advantages))
    return (
        mod_rows[0],
        (1.0 - step_len * drift_x)[0],
        step_len * vel_coef,
        (noise_level * math.sqrt(step_len))[0],
        (pg_coef * vel_coef * math.sqrt(step_len) / noise_level)[0],
        (vel_coef * vel_coef * step_len / (noise_level * noise_level))[0],
    )


def inputs_of(latent, mod_rows):
    normed = latent * lax.rsqrt(jnp.mean(latent * latent, axis=1, keepdims=True) + 1e-06)
    return (normed * (1.0 + mod_rows[1]) + mod_rows[0]).astype(jnp.bfloat16)


def forward(inputs, w_in, w_down):
    pre_act = jnp.dot(inputs, w_in, preferred_element_type=jnp.float32) / math.sqrt(
        w_in.shape[0]
    )
    hidden = gelu_parts(pre_act)[0].astype(jnp.bfloat16)
    hidden_width = w_in.shape[1] * lax.axis_size(MP)
    partial = jnp.einsum(
        "lf,df->ld", hidden, w_down, preferred_element_type=jnp.float32
    ) / math.sqrt(hidden_width)
    return pre_act, hidden, partial.astype(jnp.bfloat16)


def next_latent(latent, velocity, noise, factors):
    _, keep, pull, spread, _, _ = factors
    step_mean = latent * keep - pull * velocity.astype(jnp.float32)
    return step_mean + spread * noise.astype(jnp.float32)


def velocity_grad(velocity, noise, ref_velocity, factors):
    gap = velocity.astype(jnp.float32) - ref_velocity.astype(jnp.float32)
    return (factors[4] * noise.astype(jnp.float32) + factors[5] * gap).astype(jnp.bfloat16)


def hidden_grad(vel_grad, w_down, pre_act, hidden_width):
    wide = jnp.einsum(
        "ld,df->lf", vel_grad, w_down, preferred_element_type=jnp.float32
    ) / math.sqrt(hidden_width)
    return (wide * gelu_parts(pre_act)[1]).astype(jnp.bfloat16)


def on_device(
    latents, noise, ref_velocity, start_step, advantages, behaviour_gap, modulation, w_in, w_down
):
    model_width = latents.shape[2]
    hidden_width = w_in.shape[1] * lax.axis_size(MP)
    first, second = (
        step_factors(start_step, advantages, behaviour_gap, modulation, k) for k in range(2)
    )
    w_in_full, w_down_full = gathered_weights(w_in, w_down)
    u_0 = inputs_of(latents[0], first[0])
    pre_0, hidden_0, part_0 = forward(u_0, w_in_full, w_down_full)
    velocity_0 = join_shares(over_z(over_y(part_0)), "mp_0", 0)
    x1 = next_latent(latents[0], velocity_0, noise[0, 0], first)
    u_1 = inputs_of(x1, second[0])
    pre_1, hidden_1, part_1 = forward(u_1, w_in_full, w_down_full)
    mine, velocity_b = lax.optimization_barrier((over_y(part_1), velocity_0))
    e_0 = velocity_grad(velocity_b, noise[0, 0], ref_velocity[0, 0], first)
    e_0 = lax.optimization_barrier(e_0)
    d_0 = hidden_grad(e_0, w_down_full, pre_0, hidden_width)
    g_0, g_1 = lax.optimization_barrier((hidden_0, hidden_1))
    rows, e_0, d_0, g_0, g_1 = lax.optimization_barrier((over_z(mine), e_0, d_0, g_0, g_1))
    velocity_1 = join_shares(rows, "mp_0", 0)
    e_1 = velocity_grad(velocity_1, noise[0, 1], ref_velocity[0, 1], second)
    e_1 = lax.optimization_barrier(e_1)
    d_1 = lax.optimization_barrier(hidden_grad(e_1, w_down_full, pre_1, hidden_width))
    in_halves = grad_halves((u_0, u_1), (d_0, d_1), 1.0 / math.sqrt(model_width))
    in_halves, e_1, velocity_1 = lax.optimization_barrier((in_halves, e_1, velocity_1))
    down_halves = grad_halves((e_0, e_1), (g_0, g_1), 1.0 / math.sqrt(hidden_width))
    in_half, down_halves, velocity_1 = lax.optimization_barrier(
        (over_cores(*in_halves), down_halves, velocity_1)
    )
    in_mine = z_then_x(in_half)
    down_mine = x_then_z(over_cores(*down_halves))
    final = next_latent(x1, velocity_1, noise[0, 1], second)[None]
    total = sum_over_all(jnp.sum(in_mine * in_mine) + jnp.sum(down_mine * down_mine))
    grad_rms = jnp.sqrt(total / (2.0 * model_width * hidden_width) + 1e-06)
    new_in = (w_in.astype(jnp.float32) - in_mine / grad_rms).astype(jnp.bfloat16)
    new_down = (w_down.astype(jnp.float32) - down_mine / grad_rms).astype(jnp.bfloat16)
    return (final, new_in, new_down)


def solution(mesh):
    finer = Mesh(
        mesh.devices.reshape(mesh.shape["group"], 2, 4, 4, 4),
        ("group", "dp_0", "dp_1", "mp_0", "mp_1"),
    )
    placed = (
        P(GROUP_DP, None, None),
        P(GROUP_DP, None, None, None),
        P(GROUP_DP, None, None, None),
        P(GROUP_DP),
        P(GROUP_DP),
        P(GROUP_DP, None),
        P(),
        P(GROUP_DP, MP),
        P(GROUP_DP, MP),
    )
    return jax.shard_map(
        on_device,
        mesh=finer,
        in_specs=placed,
        out_specs=(P(GROUP_DP, None, None), P(GROUP_DP, MP), P(GROUP_DP, MP)),
        check_vma=False,
    )
```
